32 devices in a mesh: tile: 8 (over y, x, core), layer: 4 (over z).
Axes of the slice: x: 2, y: 2, z: 4, core: 2. Of those that a mesh axis runs over, the one named last changes fastest.
Arguments:
- rand_vectors: bfloat16 [4, 16, 98304], P(None, None, ('tile', 'layer')), may hold values from -4 to 4
- onsite: bfloat16 [768, 128, 128], P(('tile', 'layer')), as said below
- down_hop: bfloat16 [768, 128, 128], P(('tile', 'layer')), may hold values from -0.1875 to 0.1875
- right_hop: bfloat16 [768, 128, 128], P(('tile', 'layer')), may hold values from -0.1875 to 0.1875
- pattern: int32 [768, 2], P(('tile', 'layer')), may hold values 0 or 1
- pairing: float32 [98304], P(('tile', 'layer')), may hold values from 0.1 to 1
- link_rows: int32 [256, 8], P(('tile', 'layer')), may hold values from 0 to 3071
- link_target: int32 [256, 8], P(('tile', 'layer')), may hold values from 0 to 3071
- link_weight: bfloat16 [256, 8], P(('tile', 'layer')), may hold values from -3 to 3
- link_count: int32 [256], P(('tile', 'layer')), may hold values from 0 to 8, as said below
Outputs:
- cheb_one: float32 [4, 16, 98304], P(None, None, ('tile', 'layer'))
- cheb_two: float32 [4, 16, 98304], P(None, None, ('tile', 'layer'))
- moments: float32 [3, 4, 98304], P(None, None, ('tile', 'layer'))
The draws below stay inside these ranges and needn't reach their ends.
Inputs may be any that keep to these rules, and one draw needn't show every extreme that they name: `onsite`: every tile is symmetric. `link_rows`: a local site of the sending device. `link_target`: a local site of the receiving device. `link_count`: the number of used slots from one source tile row index to one receiving device; loads differ strongly between receiving tile row indices.
All inputs are finite; a program needn't handle non-finite values. No bound on the sum of `pattern` on one device may be relied on, other than what follows from the above.
Results may differ from the reference program's by a relative error of at most 0.0025.
Values may be sent and summed in bfloat16 or wider, within the bound.
A program may use at most 64 MiB of HBM per device.

```python
import math
import jax
import jax.numpy as jnp
from jax import lax

COMP = 4
VECS = 16
TILE = 128
TR = 4
TC = 6
CAP = 8
SD = 3072
SITES = 98304
TILES = 768
LINKS = 256
N_TILE = 8
N_LAYER = 4


def draw_onsite(key, part):
    base = jax.random.normal(key, (TILES, TILE, TILE), jnp.float32)
    base = base * (1.0 / math.sqrt(TILE))
    return ((base + jnp.swapaxes(base, 1, 2)) * 0.5).astype(jnp.bfloat16)


def draw_link_count(key, part):
    first_key, second_key, third_key = jax.random.split(key, 3)
    tile_total = math.isqrt(LINKS // 4)
    counts = jax.random.randint(first_key, (LINKS,), 0, CAP + 1, dtype=jnp.int32)
    keeper = jax.random.randint(second_key, (LINKS,), 0, 4, dtype=jnp.int32)
    counts = jnp.where(keeper > 0, counts, 0)
    hottest = jax.random.randint(third_key, (), 0, tile_total, dtype=jnp.int32)
    receiver_tile = jnp.arange(LINKS, dtype=jnp.int32) // (4 * tile_total)
    counts = jnp.where(receiver_tile == hottest, CAP, counts)
    return counts.astype(jnp.int32)


def with_ends(drawn, own_key, low, high):
    longest = drawn.shape.index(max(drawn.shape))
    spots = []
    for shift in (0, 1):
        where = [jax.random.randint(jax.random.fold_in(own_key, axis), (), 0, length) for axis, length in enumerate(drawn.shape)]
        where[longest] = (where[longest] + shift) % drawn.shape[longest]
        spots.append(tuple(where))
    return drawn.at[spots[0]].set(low).at[spots[1]].set(high)


def steps_of(rng, shape, shards, smallest, largest):
    level = 1.0
    for position, shards_of in shards:
        draws = jax.random.uniform(jax.random.fold_in(jax.random.fold_in(rng, 6), position), (shards_of,), jnp.float32, smallest / len(shards), largest / len(shards))
        level = level * jnp.repeat(jnp.exp(draws), shape[position] // shards_of).reshape((-1,) + (1,) * (len(shape) - 1 - position))
    return level


def gaussian(own_key, extent, deviation, limit, shards=(), held_as=jnp.bfloat16):
    result = deviation * jax.random.normal(own_key, extent, jnp.float32)
    if shards:
        result = result * steps_of(own_key, extent, shards, -0.22, 0.18)
    return jnp.clip(result, -limit, limit).astype(held_as)


def setup_inputs(seed: int = 0) -> dict:
    arg_keys = jax.random.split(jax.random.key(seed), 11)
    rand_vectors = gaussian(arg_keys[0], (COMP, VECS, SITES), 1.0, 4.0, ((2, 32),))
    onsite = draw_onsite(jax.random.fold_in(arg_keys[10], 71), 0)
    down_hop = gaussian(arg_keys[2], (TILES, TILE, TILE), (8 * TILE) ** -0.5, 0.1875, ((0, 32),))
    right_hop = gaussian(arg_keys[3], (TILES, TILE, TILE), (8 * TILE) ** -0.5, 0.1875, ((0, 32),))
    pattern = with_ends((jax.random.randint(arg_keys[4], (TILES, 2), 0, 4) < 3).astype(jnp.int32), jax.random.fold_in(arg_keys[4], 1), 0, 1)
    pairing = jnp.clip(jnp.exp(math.log(1.0) - 2.3025851 * jax.random.uniform(arg_keys[5], (SITES,), jnp.float32) ** steps_of(arg_keys[5], (SITES,), ((0, 32),), -0.2, 0.2)), 0.1, 1.0)
    link_rows = with_ends(jax.random.randint(arg_keys[6], (LINKS, CAP), 0, SD), jax.random.fold_in(arg_keys[6], 1), 0, SD - 1).astype(jnp.int32)
    link_target = with_ends(jax.random.randint(arg_keys[7], (LINKS, CAP), 0, SD), jax.random.fold_in(arg_keys[7], 1), 0, SD - 1).astype(jnp.int32)
    link_weight = gaussian(arg_keys[8], (LINKS, CAP), 0.5, 3.0, ((0, 32),))
    link_count = draw_link_count(jax.random.fold_in(arg_keys[10], 71), 0)
    return {"rand_vectors": rand_vectors, "onsite": onsite, "down_hop": down_hop, "right_hop": right_hop, "pattern": pattern, "pairing": pairing, "link_rows": link_rows, "link_target": link_target, "link_weight": link_weight, "link_count": link_count}


FORWARD_FORM = "kij,nkj->nki"
TRANSPOSED_FORM = "kji,nkj->nki"


def tile_rows(tiles, field_grid, einsum_form):
    def row_product(row_pair):
        block_tiles, field_row = row_pair
        return jnp.einsum(einsum_form, block_tiles.astype(jnp.float32), field_row.astype(jnp.float32))

    mapped = lax.map(row_product, (tiles, jnp.moveaxis(field_grid, 1, 0)))
    return jnp.moveaxis(mapped, 0, 1)


def layer_tiles(tiles, layer_index):
    sixfold = tiles.reshape(N_TILE, N_LAYER, TR, TC, TILE, TILE)[:, 2 * layer_index:2 * layer_index + 2]
    return sixfold.transpose(0, 2, 1, 3, 4, 5).reshape(N_TILE * TR, 2 * TC, TILE, TILE)


def layer_field(field, layer_index):
    field_rows = field.shape[0]
    sixfold = field.reshape(field_rows, N_TILE, N_LAYER, TR, TC, TILE)[:, :, 2 * layer_index:2 * layer_index + 2]
    return sixfold.transpose(0, 1, 3, 2, 4, 5).reshape(field_rows, N_TILE * TR, 2 * TC, TILE)


def intra_layer(field_b, self_tiles, down_mask, right_mask):
    field_rows = field_b.shape[0]
    pieces = []
    for layer_index in range(2):
        field_grid = layer_field(field_b, layer_index)
        onsite_grid = layer_tiles(self_tiles, layer_index)
        down_grid = layer_tiles(down_mask, layer_index)
        right_grid = layer_tiles(right_mask, layer_index)
        zero_row = jnp.zeros_like(field_grid[:, :1])
        zero_column = jnp.zeros_like(field_grid[:, :, :1])
        result_grid = tile_rows(onsite_grid, field_grid, FORWARD_FORM)
        result_grid = result_grid + tile_rows(down_grid, jnp.concatenate([field_grid[:, 1:], zero_row], axis=1), FORWARD_FORM)
        upward = tile_rows(down_grid, field_grid, TRANSPOSED_FORM)
        result_grid = result_grid + jnp.concatenate([jnp.zeros_like(upward[:, :1]), upward[:, :-1]], axis=1)
        result_grid = result_grid + tile_rows(right_grid, jnp.concatenate([field_grid[:, :, 1:], zero_column], axis=2), FORWARD_FORM)
        leftward = tile_rows(right_grid, field_grid, TRANSPOSED_FORM)
        result_grid = result_grid + jnp.concatenate([jnp.zeros_like(leftward[:, :, :1]), leftward[:, :, :-1]], axis=2)
        pieces.append(result_grid.reshape(field_rows, N_TILE, TR, 2, TC, TILE).transpose(0, 1, 3, 2, 4, 5))
    return jnp.concatenate(pieces, axis=2).reshape(field_rows, SITES)


def inter_layer(field_b, link_rows, link_target, link_weight, link_count):
    columns = field_b.T
    flipped = jnp.array([2, 3, 0, 1], dtype=jnp.int32)
    sent_rows = link_rows.reshape(N_TILE, N_LAYER, N_TILE, CAP)[:, flipped].transpose(2, 1, 0, 3)
    slot_live = jnp.arange(CAP, dtype=jnp.int32).reshape(1, 1, 1, CAP) < link_count.reshape(N_TILE, N_LAYER, N_TILE, 1)
    slot_weight = jnp.where(slot_live, link_weight.reshape(N_TILE, N_LAYER, N_TILE, CAP).astype(jnp.float32), 0.0).reshape(-1, 1)
    tile_index = jnp.arange(N_TILE, dtype=jnp.int32).reshape(N_TILE, 1, 1, 1)
    layer_index = jnp.arange(N_LAYER, dtype=jnp.int32).reshape(1, N_LAYER, 1, 1)
    source_tile = jnp.arange(N_TILE, dtype=jnp.int32).reshape(1, 1, N_TILE, 1)
    receiver = ((tile_index * N_LAYER + layer_index) * SD + link_target.reshape(N_TILE, N_LAYER, N_TILE, CAP)).astype(jnp.int32).reshape(-1)
    sender = ((source_tile * N_LAYER + (layer_index + 2) % N_LAYER) * SD + sent_rows).astype(jnp.int32).reshape(-1)
    forward = jnp.take(columns, sender, axis=0).astype(jnp.float32) * slot_weight
    backward = jnp.take(columns, receiver, axis=0).astype(jnp.float32) * slot_weight
    summed = jax.ops.segment_sum(forward, receiver, num_segments=SITES) + jax.ops.segment_sum(backward, sender, num_segments=SITES)
    return summed.T


def reference(rand_vectors, onsite, down_hop, right_hop, pattern, pairing, link_rows, link_target, link_weight, link_count):
    down_mask = down_hop * pattern[:, 0][:, None, None].astype(jnp.bfloat16)
    right_mask = right_hop * pattern[:, 1][:, None, None].astype(jnp.bfloat16)
    nambu_sign = jnp.array([1.0, 1.0, -1.0, -1.0], dtype=jnp.float32)[:, None, None]
    field_rows = COMP * VECS

    def apply_hop(field_b):
        flat_field = field_b.reshape(field_rows, SITES)
        summed = intra_layer(flat_field, onsite, down_mask, right_mask) + inter_layer(flat_field, link_rows, link_target, link_weight, link_count)
        return summed.reshape(COMP, VECS, SITES)

    initial = rand_vectors.astype(jnp.float32)
    cheb_one = nambu_sign * apply_hop(rand_vectors) + pairing * jnp.roll(initial, 2, axis=0)
    one_rounded = cheb_one.astype(jnp.bfloat16)
    cheb_two = 2.0 * (nambu_sign * apply_hop(one_rounded) + pairing * jnp.roll(cheb_one, 2, axis=0)) - initial
    moments = jnp.stack([jnp.mean(initial * initial, axis=1), jnp.mean(initial * cheb_one, axis=1), jnp.mean(initial * cheb_two, axis=1)])
    return cheb_one, cheb_two, moments
```

```python
import functools

import jax
import jax.numpy as jnp
from jax import lax
from jax.experimental import pallas as pl
from jax.experimental.pallas import tpu as pltpu
from jax.sharding import PartitionSpec as P

TR = 4
TC = 6
MESH = pl.DeviceIdType.MESH
F32 = jnp.float32
BF16 = jnp.bfloat16


def dot_nn(a, b):
    return lax.dot_general(a, b, (((1,), (0,)), ((), ())), preferred_element_type=F32)


def dot_nt(a, b):
    return lax.dot_general(a, b, (((1,), (1,)), ((), ())), preferred_element_type=F32)


def each(count, body):
    if count <= 16:
        for i in range(count):
            body(i)
    else:

        def step(i, carry):
            body(i)
            return carry

        lax.fori_loop(0, count, step, 0)


def kernel(
    n,
    nl,
    x_hbm,
    on_hbm,
    down_hbm,
    right_hbm,
    pat_ref,
    pair_ref,
    rows_ref,
    target_ref,
    weight_ref,
    count_ref,
    one_ref,
    two_ref,
    mom_ref,
    x_ref,
    on_ref,
    down_ref,
    right_ref,
    acc_ref,
    oneb_ref,
    hot_ref,
    idx_ref,
    wsend_ref,
    wloc_ref,
    gath_ref,
    wide_ref,
    sbuf,
    lbuf,
    pbuf,
    low_in,
    up_in,
    cbuf,
    col_in,
    load_sem,
    link_send,
    link_recv,
    edge_send,
    edge_recv,
):
    t = lax.axis_index("tile")
    l = lax.axis_index("layer")
    far = lax.rem(l + nl // 2, nl)
    is_left = lax.rem(l, 2) == 0
    partner = l + 1 - 2 * lax.rem(l, 2)
    fr, sites = x_ref.shape
    tile = on_ref.shape[1]
    tiles = sites // tile
    cap = rows_ref.shape[1]
    slots = n * 2 * cap
    wide = TC * tile

    loads = [
        pltpu.make_async_copy(x_hbm, x_ref, load_sem.at[0]),
        pltpu.make_async_copy(down_hbm, down_ref, load_sem.at[1]),
        pltpu.make_async_copy(right_hbm, right_ref, load_sem.at[2]),
        pltpu.make_async_copy(on_hbm, on_ref, load_sem.at[3]),
    ]
    for load in loads:
        load.start()

    has_up = t > 0
    has_low = t < n - 1
    barrier = pltpu.get_barrier_semaphore()
    each(
        n,
        lambda s: pl.semaphore_signal(barrier, inc=1, device_id=(s, far), device_id_type=MESH),
    )
    pl.semaphore_signal(barrier, inc=1, device_id=(t, partner), device_id_type=MESH)

    @pl.when(has_up)
    def _():
        pl.semaphore_signal(barrier, inc=1, device_id=(t - 1, l), device_id_type=MESH)

    @pl.when(has_low)
    def _():
        pl.semaphore_signal(barrier, inc=1, device_id=(t + 1, l), device_id_type=MESH)

    @pl.when(jnp.logical_not(has_up))
    def _():
        up_in[...] = jnp.zeros_like(up_in)

    @pl.when(jnp.logical_not(has_low))
    def _():
        low_in[...] = jnp.zeros_like(low_in)

    sub = lax.broadcasted_iota(jnp.int32, (cap, cap), 0)
    lane = lax.broadcasted_iota(jnp.int32, (cap, cap), 1)
    eye = sub == lane
    half = lax.broadcasted_iota(jnp.int32, (cap, 2 * fr), 1) >= fr

    wide_ref[...] = weight_ref[...].astype(F32)

    def columns(s):
        def column(row):
            spread = jnp.broadcast_to(row.astype(F32), (cap, cap))
            return jnp.sum(jnp.where(eye, spread, 0.0), axis=1, keepdims=True)

        base = s * (2 * cap)
        out_col = column(rows_ref[pl.ds(s, 1), :])
        own_col = column(target_ref[pl.ds(s, 1), :])
        idx_ref[pl.ds(base, cap), :] = jnp.broadcast_to(out_col, (cap, tile)).astype(jnp.int32)
        idx_ref[pl.ds(base + cap, cap), :] = jnp.broadcast_to(own_col, (cap, tile)).astype(
            jnp.int32
        )
        live = lax.broadcasted_iota(jnp.int32, (1, cap), 1) < count_ref[s]
        w_col = column(jnp.where(live, wide_ref[pl.ds(s, 1), :], 0.0))
        w_wide = jnp.where(half, jnp.broadcast_to(w_col, (cap, 2 * fr)), 0.0)
        zero = jnp.zeros_like(w_wide)
        wsend_ref[pl.ds(base, cap), :] = w_wide
        wsend_ref[pl.ds(base + cap, cap), :] = zero
        wloc_ref[pl.ds(base, cap), :] = zero
        wloc_ref[pl.ds(base + cap, cap), :] = w_wide

    each(n, columns)
    gath_ref[...] = jnp.zeros_like(gath_ref)

    lanes = lax.broadcasted_iota(jnp.int32, (slots, tile), 1)
    for p in range(tiles):
        hot = jnp.where(idx_ref[...] == lanes + p * tile, 1.0, 0.0)
        hot_ref[:, p * tile : (p + 1) * tile] = hot.astype(BF16)

    def block(ref, p):
        return ref[:, p * tile : (p + 1) * tile]

    def link_copy(rd, s, mine):
        return pltpu.make_async_remote_copy(
            src_ref=sbuf.at[rd, s],
            dst_ref=lbuf.at[rd, mine],
            send_sem=link_send.at[rd, s],
            recv_sem=link_recv.at[rd, mine],
            device_id=(s, far),
            device_id_type=MESH,
        )

    def field_copy(rd, src):
        return pltpu.make_async_remote_copy(
            src_ref=src.at[:, 0:wide],
            dst_ref=low_in.at[rd],
            send_sem=edge_send.at[rd, 0],
            recv_sem=edge_recv.at[rd, 0],
            device_id=(t - 1, l),
            device_id_type=MESH,
        )

    def partial_copy(rd):
        return pltpu.make_async_remote_copy(
            src_ref=pbuf.at[rd],
            dst_ref=up_in.at[rd],
            send_sem=edge_send.at[rd, 1],
            recv_sem=edge_recv.at[rd, 1],
            device_id=(t + 1, l),
            device_id_type=MESH,
        )

    def column_copy(rd):
        return pltpu.make_async_remote_copy(
            src_ref=cbuf.at[rd],
            dst_ref=col_in.at[rd],
            send_sem=edge_send.at[rd, 2],
            recv_sem=edge_recv.at[rd, 2],
            device_id=(t, partner),
            device_id_type=MESH,
        )

    def gather(rd, src):
        gath_ref[:, 0:fr] = dot_nt(hot_ref[...], src[...])

        def fill(s):
            base = s * (2 * cap)
            both = jnp.concatenate(
                [gath_ref[pl.ds(base + cap, cap), :], gath_ref[pl.ds(base, cap), :]], axis=0
            )
            sbuf[rd, s] = (both + wsend_ref[pl.ds(base, 2 * cap), :]).astype(BF16)

        each(n, fill)

    def edges(rd, src):
        for k in range(TC):
            p = (TR - 1) * TC + k
            pbuf[rd, :, k * tile : (k + 1) * tile] = dot_nn(block(src, p), down_ref[p]).astype(
                BF16
            )
        for r in range(TR):
            p = r * TC + TC - 1
            passed = dot_nn(block(src, p), right_ref[p])
            own = block(src, r * TC).astype(F32)
            cbuf[rd, :, r * tile : (r + 1) * tile] = jnp.where(is_left, passed, own).astype(BF16)

    def send_links(rd):
        each(n, lambda s: link_copy(rd, s, t).start())

    def send_edges(rd, src):
        column_copy(rd).start()

        @pl.when(has_up)
        def _():
            field_copy(rd, src).start()

        @pl.when(has_low)
        def _():
            partial_copy(rd).start()

    def local(src):
        for r in range(TR):
            for k in range(TC):
                p = r * TC + k
                ins = [block(src, p)]
                mats = [on_ref[p]]
                if r > 0:
                    ins.append(block(src, p - TC))
                    mats.append(down_ref[p - TC])
                if k > 0:
                    ins.append(block(src, p - 1))
                    mats.append(right_ref[p - 1])
                total = dot_nn(jnp.concatenate(ins, axis=1), jnp.concatenate(mats, axis=0))
                ins, mats = [], []
                if r < TR - 1:
                    ins.append(block(src, p + TC))
                    mats.append(down_ref[p])
                if k < TC - 1:
                    ins.append(block(src, p + 1))
                    mats.append(right_ref[p])
                if ins:
                    total = total + dot_nt(
                        jnp.concatenate(ins, axis=1), jnp.concatenate(mats, axis=1)
                    )
                acc_ref[:, p * tile : (p + 1) * tile] = total

    def receive_edges(rd):
        @pl.when(has_low)
        def _():
            field_copy(rd, x_ref).wait_recv()

        @pl.when(has_up)
        def _():
            partial_copy(rd).wait_recv()

        column_copy(rd).wait_recv()

    def add_edges(rd):
        for k in range(TC):
            cols = slice(k * tile, (k + 1) * tile)
            acc_ref[:, cols] += up_in[rd, :, cols].astype(F32)
            p = (TR - 1) * TC + k
            acc_ref[:, p * tile : (p + 1) * tile] += dot_nt(low_in[rd, :, cols], down_ref[p])
        for r in range(TR):
            arrived = col_in[rd, :, r * tile : (r + 1) * tile].astype(F32)
            p = r * TC
            acc_ref[:, p * tile : (p + 1) * tile] += jnp.where(is_left, 0.0, arrived)
            p = r * TC + TC - 1
            field = jnp.where(is_left, arrived, 0.0).astype(BF16)
            acc_ref[:, p * tile : (p + 1) * tile] += dot_nt(field, right_ref[p])

    def link_terms(rd):
        each(n, lambda s: link_copy(rd, s, s).wait_recv())
        landed = lbuf[rd].reshape(slots, 2 * fr).astype(F32) + wloc_ref[...]
        turned = landed.T
        terms = turned[0:fr] * turned[fr : 2 * fr]
        high = terms.astype(BF16)
        low = (terms - high.astype(F32)).astype(BF16)
        return jnp.concatenate([high, low], axis=0)

    sign = jnp.where(lax.broadcasted_iota(jnp.int32, (fr, tile), 0) < fr // 2, 1.0, -1.0)

    def flipped(v):
        return jnp.concatenate([v[fr // 2 :], v[: fr // 2]], axis=0)

    def scattered(terms, p):
        both = dot_nn(terms, block(hot_ref, p))
        return both[0:fr] + both[fr : 2 * fr]

    loads[0].wait()
    gather(0, x_ref)
    loads[1].wait()
    loads[2].wait()
    for p in range(tiles):
        down_ref[p] = down_ref[p] * pat_ref[p, 0].astype(F32).astype(BF16)
        right_ref[p] = right_ref[p] * pat_ref[p, 1].astype(F32).astype(BF16)
    edges(0, x_ref)
    pl.semaphore_wait(barrier, n + 1 + has_up.astype(jnp.int32) + has_low.astype(jnp.int32))
    send_links(0)
    send_edges(0, x_ref)
    loads[3].wait()
    local(x_ref)
    receive_edges(0)
    add_edges(0)
    terms = link_terms(0)
    for p in range(tiles):
        cols = slice(p * tile, (p + 1) * tile)
        hop = acc_ref[:, cols] + scattered(terms, p)
        start = x_ref[:, cols].astype(F32)
        one = sign * hop + pair_ref[:, cols] * flipped(start)
        one_ref[:, cols] = one
        oneb_ref[:, cols] = one.astype(BF16)

    gather(1, oneb_ref)
    send_links(1)
    edges(1, oneb_ref)
    send_edges(1, oneb_ref)
    local(oneb_ref)
    receive_edges(1)
    add_edges(1)
    terms = link_terms(1)
    comps, vecs = mom_ref.shape[1], fr // mom_ref.shape[1]

    def mean(v):
        return jnp.sum(v.reshape(comps, vecs, tile), axis=1) * (1.0 / vecs)

    for p in range(tiles):
        cols = slice(p * tile, (p + 1) * tile)
        hop = acc_ref[:, cols] + scattered(terms, p)
        start = x_ref[:, cols].astype(F32)
        one = one_ref[:, cols]
        two = 2.0 * (sign * hop + pair_ref[:, cols] * flipped(one)) - start
        two_ref[:, cols] = two
        mom_ref[0, :, cols] = mean(start * start)
        mom_ref[1, :, cols] = mean(start * one)
        mom_ref[2, :, cols] = mean(start * two)

    for rd in range(2):
        each(n, lambda s: link_copy(rd, s, t).wait_send())
        column_copy(rd).wait_send()

        @pl.when(has_up)
        def _():
            field_copy(rd, x_ref).wait_send()

        @pl.when(has_low)
        def _():
            partial_copy(rd).wait_send()


def shards(
    n,
    nl,
    rand_vectors,
    onsite,
    down_hop,
    right_hop,
    pattern,
    pairing,
    link_rows,
    link_target,
    link_weight,
    link_count,
):
    comps, vecs, sites = rand_vectors.shape
    fr = comps * vecs
    tiles, tile, _ = onsite.shape
    cap = link_rows.shape[1]
    slots = 2 * n * cap
    wide, tall = TC * tile, TR * tile
    vmem = pl.BlockSpec(memory_space=pltpu.VMEM)
    smem = pl.BlockSpec(memory_space=pltpu.SMEM)
    hbm = pl.BlockSpec(memory_space=pl.ANY)
    one, two, moments = pl.pallas_call(
        functools.partial(kernel, n, nl),
        out_shape=(
            jax.ShapeDtypeStruct((fr, sites), F32),
            jax.ShapeDtypeStruct((fr, sites), F32),
            jax.ShapeDtypeStruct((3, comps, sites), F32),
        ),
        in_specs=[hbm, hbm, hbm, hbm, smem, vmem, vmem, vmem, vmem, smem],
        out_specs=(vmem, vmem, vmem),
        scratch_shapes=[
            pltpu.VMEM((fr, sites), BF16),
            pltpu.VMEM((tiles, tile, tile), BF16),
            pltpu.VMEM((tiles, tile, tile), BF16),
            pltpu.VMEM((tiles, tile, tile), BF16),
            pltpu.VMEM((fr, sites), F32),
            pltpu.VMEM((fr, sites), BF16),
            pltpu.VMEM((slots, sites), BF16),
            pltpu.VMEM((slots, tile), jnp.int32),
            pltpu.VMEM((slots, 2 * fr), F32),
            pltpu.VMEM((slots, 2 * fr), F32),
            pltpu.VMEM((slots, 2 * fr), F32),
            pltpu.VMEM((n, cap), F32),
            pltpu.VMEM((2, n, 2 * cap, 2 * fr), BF16),
            pltpu.VMEM((2, n, 2 * cap, 2 * fr), BF16),
            pltpu.VMEM((2, fr, wide), BF16),
            pltpu.VMEM((2, fr, wide), BF16),
            pltpu.VMEM((2, fr, wide), BF16),
            pltpu.VMEM((2, fr, tall), BF16),
            pltpu.VMEM((2, fr, tall), BF16),
            pltpu.SemaphoreType.DMA((4,)),
            pltpu.SemaphoreType.DMA((2, n)),
            pltpu.SemaphoreType.DMA((2, n)),
            pltpu.SemaphoreType.DMA((2, 3)),
            pltpu.SemaphoreType.DMA((2, 3)),
        ],
        compiler_params=pltpu.CompilerParams(
            collective_id=0, has_side_effects=True, vmem_limit_bytes=56 * 1024 * 1024
        ),
    )(
        rand_vectors.reshape(fr, sites),
        onsite,
        down_hop,
        right_hop,
        pattern,
        pairing.reshape(1, sites),
        link_rows,
        link_target,
        link_weight,
        link_count,
    )
    return (
        one.reshape(comps, vecs, sites),
        two.reshape(comps, vecs, sites),
        moments,
    )


def solution(mesh):
    spread = ("tile", "layer")
    in_specs = (
        P(None, None, spread),
        P(spread, None, None),
        P(spread, None, None),
        P(spread, None, None),
        P(spread, None),
        P(spread),
        P(spread, None),
        P(spread, None),
        P(spread, None),
        P(spread),
    )
    out_specs = (P(None, None, spread),) * 3
    return jax.shard_map(
        functools.partial(shards, mesh.shape["tile"], mesh.shape["layer"]),
        mesh=mesh,
        in_specs=in_specs,
        out_specs=out_specs,
        check_vma=False,
    )
```

```python
import functools

import jax
import jax.numpy as jnp
from jax import lax
from jax.experimental import pallas as pl
from jax.experimental.pallas import tpu as pltpu
from jax.sharding import PartitionSpec as P

TR = 4
TC = 6
MESH = pl.DeviceIdType.MESH
F32 = jnp.float32
BF16 = jnp.bfloat16


def dot_nn(a, b):
    return lax.dot_general(a, b, (((1,), (0,)), ((), ())), preferred_element_type=F32)


def dot_nt(a, b):
    return lax.dot_general(a, b, (((1,), (1,)), ((), ())), preferred_element_type=F32)


def mean(v, comps, vecs):
    return jnp.sum(v.reshape(comps, vecs, v.shape[1]), axis=1) * (1.0 / vecs)


def each(count, body):
    if count <= 16:
        for i in range(count):
            body(i)
    else:

        def step(i, carry):
            body(i)
            return carry

        lax.fori_loop(0, count, step, 0)


def kernel(
    n,
    nl,
    x_hbm,
    on_hbm,
    down_hbm,
    right_hbm,
    pat_hbm,
    pair_hbm,
    rows_hbm,
    target_hbm,
    weight_hbm,
    count_hbm,
    x_ref,
    one_ref,
    acc_ref,
    hot_ref,
    terms_ref,
    mom_ref,
    pat_ref,
    pair_ref,
    rows_ref,
    target_ref,
    weight_ref,
    count_ref,
    on_ref,
    down_ref,
    right_ref,
    oneb_ref,
    idx_ref,
    wsend_ref,
    wloc_ref,
    gath_ref,
    wide_ref,
    sbuf,
    lbuf,
    pbuf,
    low_in,
    up_in,
    cbuf,
    col_in,
    load_sem,
    link_send,
    link_recv,
    edge_send,
    edge_recv,
):
    t = lax.axis_index("tile")
    l = lax.axis_index("layer")
    far = lax.rem(l + nl // 2, nl)
    is_left = lax.rem(l, 2) == 0
    partner = l + 1 - 2 * lax.rem(l, 2)
    fr, sites = x_ref.shape
    tile = on_ref.shape[1]
    tiles = sites // tile
    cap = rows_ref.shape[1]
    slots = n * 2 * cap
    wide = TC * tile

    has_up = t > 0
    has_low = t < n - 1
    barrier = pltpu.get_barrier_semaphore()
    each(
        n,
        lambda s: pl.semaphore_signal(barrier, inc=1, device_id=(s, far), device_id_type=MESH),
    )
    pl.semaphore_signal(barrier, inc=1, device_id=(t, partner), device_id_type=MESH)

    @pl.when(has_up)
    def _():
        pl.semaphore_signal(barrier, inc=1, device_id=(t - 1, l), device_id_type=MESH)

    @pl.when(has_low)
    def _():
        pl.semaphore_signal(barrier, inc=1, device_id=(t + 1, l), device_id_type=MESH)

    moved = (
        (rows_hbm, rows_ref),
        (target_hbm, target_ref),
        (weight_hbm, weight_ref),
        (count_hbm, count_ref),
        (x_hbm, x_ref),
        (pat_hbm, pat_ref),
        (down_hbm, down_ref),
        (right_hbm, right_ref),
        (on_hbm, on_ref),
        (pair_hbm, pair_ref),
    )
    loads = [pltpu.make_async_copy(a, b, load_sem.at[i]) for i, (a, b) in enumerate(moved)]
    for load in loads:
        load.start()

    @pl.when(jnp.logical_not(has_up))
    def _():
        up_in[...] = jnp.zeros_like(up_in)

    @pl.when(jnp.logical_not(has_low))
    def _():
        low_in[...] = jnp.zeros_like(low_in)

    for load in loads[0:4]:
        load.wait()

    sub = lax.broadcasted_iota(jnp.int32, (cap, cap), 0)
    lane = lax.broadcasted_iota(jnp.int32, (cap, cap), 1)
    eye = sub == lane
    half = lax.broadcasted_iota(jnp.int32, (cap, 2 * fr), 1) >= fr

    wide_ref[...] = weight_ref[...].astype(F32)

    def columns(s):
        def column(row):
            spread = jnp.broadcast_to(row.astype(F32), (cap, cap))
            return jnp.sum(jnp.where(eye, spread, 0.0), axis=1, keepdims=True)

        base = s * (2 * cap)
        out_col = column(rows_ref[pl.ds(s, 1), :])
        own_col = column(target_ref[pl.ds(s, 1), :])
        idx_ref[pl.ds(base, cap), :] = jnp.broadcast_to(out_col, (cap, tile)).astype(jnp.int32)
        idx_ref[pl.ds(base + cap, cap), :] = jnp.broadcast_to(own_col, (cap, tile)).astype(
            jnp.int32
        )
        live = lax.broadcasted_iota(jnp.int32, (1, cap), 1) < count_ref[s]
        w_col = column(jnp.where(live, wide_ref[pl.ds(s, 1), :], 0.0))
        w_wide = jnp.where(half, jnp.broadcast_to(w_col, (cap, 2 * fr)), 0.0)
        zero = jnp.zeros_like(w_wide)
        wsend_ref[pl.ds(base, cap), :] = w_wide
        wsend_ref[pl.ds(base + cap, cap), :] = zero
        wloc_ref[pl.ds(base, cap), :] = zero
        wloc_ref[pl.ds(base + cap, cap), :] = w_wide

    each(n, columns)
    gath_ref[...] = jnp.zeros_like(gath_ref)

    lanes = lax.broadcasted_iota(jnp.int32, (slots, tile), 1)
    for p in range(tiles):
        hot = jnp.where(idx_ref[...] == lanes + p * tile, 1.0, 0.0)
        hot_ref[:, p * tile : (p + 1) * tile] = hot.astype(BF16)

    def block(ref, p):
        return ref[:, p * tile : (p + 1) * tile]

    def link_copy(rd, s, mine):
        return pltpu.make_async_remote_copy(
            src_ref=sbuf.at[rd, s],
            dst_ref=lbuf.at[rd, mine],
            send_sem=link_send.at[rd, s],
            recv_sem=link_recv.at[rd, mine],
            device_id=(s, far),
            device_id_type=MESH,
        )

    def field_copy(rd, src):
        return pltpu.make_async_remote_copy(
            src_ref=src.at[:, 0:wide],
            dst_ref=low_in.at[rd],
            send_sem=edge_send.at[rd, 0],
            recv_sem=edge_recv.at[rd, 0],
            device_id=(t - 1, l),
            device_id_type=MESH,
        )

    def partial_copy(rd):
        return pltpu.make_async_remote_copy(
            src_ref=pbuf.at[rd],
            dst_ref=up_in.at[rd],
            send_sem=edge_send.at[rd, 1],
            recv_sem=edge_recv.at[rd, 1],
            device_id=(t + 1, l),
            device_id_type=MESH,
        )

    def column_copy(rd):
        return pltpu.make_async_remote_copy(
            src_ref=cbuf.at[rd],
            dst_ref=col_in.at[rd],
            send_sem=edge_send.at[rd, 2],
            recv_sem=edge_recv.at[rd, 2],
            device_id=(t, partner),
            device_id_type=MESH,
        )

    def gather(rd, src):
        gath_ref[:, 0:fr] = dot_nt(hot_ref[...], src[...])

        def fill(s):
            base = s * (2 * cap)
            both = jnp.concatenate(
                [gath_ref[pl.ds(base + cap, cap), :], gath_ref[pl.ds(base, cap), :]], axis=0
            )
            sbuf[rd, s] = (both + wsend_ref[pl.ds(base, 2 * cap), :]).astype(BF16)

        each(n, fill)

    def edges(rd, src):
        for k in range(TC):
            p = (TR - 1) * TC + k
            pbuf[rd, :, k * tile : (k + 1) * tile] = dot_nn(block(src, p), down_ref[p]).astype(
                BF16
            )
        for r in range(TR):
            p = r * TC + TC - 1
            passed = dot_nn(block(src, p), right_ref[p])
            own = block(src, r * TC).astype(F32)
            cbuf[rd, :, r * tile : (r + 1) * tile] = jnp.where(is_left, passed, own).astype(BF16)

    def send_links(rd):
        each(n, lambda s: link_copy(rd, s, t).start())

    def send_edges(rd, src):
        column_copy(rd).start()

        @pl.when(has_up)
        def _():
            field_copy(rd, src).start()

        @pl.when(has_low)
        def _():
            partial_copy(rd).start()

    def local(src):
        for r in range(TR):
            for k in range(TC):
                p = r * TC + k
                ins = [block(src, p)]
                mats = [on_ref[p]]
                if r > 0:
                    ins.append(block(src, p - TC))
                    mats.append(down_ref[p - TC])
                if k > 0:
                    ins.append(block(src, p - 1))
                    mats.append(right_ref[p - 1])
                total = dot_nn(jnp.concatenate(ins, axis=1), jnp.concatenate(mats, axis=0))
                ins, mats = [], []
                if r < TR - 1:
                    ins.append(block(src, p + TC))
                    mats.append(down_ref[p])
                if k < TC - 1:
                    ins.append(block(src, p + 1))
                    mats.append(right_ref[p])
                if ins:
                    total = total + dot_nt(
                        jnp.concatenate(ins, axis=1), jnp.concatenate(mats, axis=1)
                    )
                acc_ref[:, p * tile : (p + 1) * tile] = total

    def receive_edges(rd):
        @pl.when(has_low)
        def _():
            field_copy(rd, x_ref).wait_recv()

        @pl.when(has_up)
        def _():
            partial_copy(rd).wait_recv()

        column_copy(rd).wait_recv()

    def add_edges(rd):
        for k in range(TC):
            cols = slice(k * tile, (k + 1) * tile)
            acc_ref[:, cols] += up_in[rd, :, cols].astype(F32)
            p = (TR - 1) * TC + k
            acc_ref[:, p * tile : (p + 1) * tile] += dot_nt(low_in[rd, :, cols], down_ref[p])
        for r in range(TR):
            arrived = col_in[rd, :, r * tile : (r + 1) * tile].astype(F32)
            p = r * TC
            acc_ref[:, p * tile : (p + 1) * tile] += jnp.where(is_left, 0.0, arrived)
            p = r * TC + TC - 1
            field = jnp.where(is_left, arrived, 0.0).astype(BF16)
            acc_ref[:, p * tile : (p + 1) * tile] += dot_nt(field, right_ref[p])

    def link_terms(rd):
        each(n, lambda s: link_copy(rd, s, s).wait_recv())
        landed = lbuf[rd].reshape(slots, 2 * fr).astype(F32) + wloc_ref[...]
        turned = landed.T
        terms = turned[0:fr] * turned[fr : 2 * fr]
        high = terms.astype(BF16)
        low = (terms - high.astype(F32)).astype(BF16)
        return jnp.concatenate([high, low], axis=0)

    sign = jnp.where(lax.broadcasted_iota(jnp.int32, (fr, tile), 0) < fr // 2, 1.0, -1.0)

    def flipped(v):
        return jnp.concatenate([v[fr // 2 :], v[: fr // 2]], axis=0)

    def scattered(terms, p):
        both = dot_nn(terms, block(hot_ref, p))
        return both[0:fr] + both[fr : 2 * fr]

    loads[4].wait()
    gather(0, x_ref)
    for load in loads[5:8]:
        load.wait()
    for p in range(tiles):
        down_ref[p] = down_ref[p] * pat_ref[0, p].astype(F32).astype(BF16)
        right_ref[p] = right_ref[p] * pat_ref[1, p].astype(F32).astype(BF16)
    edges(0, x_ref)
    pl.semaphore_wait(barrier, n + 1 + has_up.astype(jnp.int32) + has_low.astype(jnp.int32))
    send_links(0)
    send_edges(0, x_ref)
    loads[8].wait()
    loads[9].wait()
    local(x_ref)
    receive_edges(0)
    add_edges(0)
    terms = link_terms(0)
    for p in range(tiles):
        cols = slice(p * tile, (p + 1) * tile)
        hop = acc_ref[:, cols] + scattered(terms, p)
        start = x_ref[:, cols].astype(F32)
        one = sign * hop + pair_ref[:, cols] * flipped(start)
        one_ref[:, cols] = one
        oneb_ref[:, cols] = one.astype(BF16)

    gather(1, oneb_ref)
    send_links(1)
    edges(1, oneb_ref)
    send_edges(1, oneb_ref)
    local(oneb_ref)
    comps, vecs = mom_ref.shape[1], fr // mom_ref.shape[1]
    for p in range(tiles):
        cols = slice(p * tile, (p + 1) * tile)
        start = x_ref[:, cols].astype(F32)
        mom_ref[0, :, cols] = mean(start * start, comps, vecs)
        mom_ref[1, :, cols] = mean(start * one_ref[:, cols], comps, vecs)
    receive_edges(1)
    add_edges(1)
    for p in range(tiles):
        cols = slice(p * tile, (p + 1) * tile)
        start = x_ref[:, cols].astype(F32)
        own = sign * acc_ref[:, cols] + pair_ref[:, cols] * flipped(one_ref[:, cols])
        acc_ref[:, cols] = 2.0 * own - start
    terms_ref[...] = link_terms(1)

    for rd in range(2):
        each(n, lambda s: link_copy(rd, s, t).wait_send())
        column_copy(rd).wait_send()

        @pl.when(has_up)
        def _():
            field_copy(rd, x_ref).wait_send()

        @pl.when(has_low)
        def _():
            partial_copy(rd).wait_send()


def finish(
    x_ref,
    one_ref,
    acc_ref,
    hot_ref,
    terms_ref,
    mom_ref,
    one_out,
    two_out,
    mom_out,
    two_ref,
    last_ref,
    sem,
):
    fr, sites = x_ref.shape
    comps, vecs = mom_ref.shape[1], fr // mom_ref.shape[1]
    tile = sites // (TR * TC)
    wide = TC * tile
    copies = [
        pltpu.make_async_copy(one_ref, one_out, sem.at[0]),
        pltpu.make_async_copy(mom_ref, mom_out.at[0:2], sem.at[1]),
    ]
    for copy in copies:
        copy.start()
    sign = jnp.where(lax.broadcasted_iota(jnp.int32, (fr, tile), 0) < fr // 2, 2.0, -2.0)
    terms = terms_ref[...]
    for r in range(TR):
        for k in range(TC):
            p = r * TC + k
            cols = slice(p * tile, (p + 1) * tile)
            both = dot_nn(terms, hot_ref[:, cols])
            two = acc_ref[:, cols] + sign * (both[0:fr] + both[fr : 2 * fr])
            two_ref[:, cols] = two
            last_ref[:, cols] = mean(x_ref[:, cols].astype(F32) * two, comps, vecs)
        row = slice(r * wide, (r + 1) * wide)
        copy = pltpu.make_async_copy(two_ref.at[:, row], two_out.at[:, row], sem.at[2 + r])
        copy.start()
        copies.append(copy)
    copy = pltpu.make_async_copy(last_ref, mom_out.at[2], sem.at[2 + TR])
    copy.start()
    copies.append(copy)
    for copy in copies:
        copy.wait()


def shards(
    n,
    nl,
    rand_vectors,
    onsite,
    down_hop,
    right_hop,
    pattern,
    pairing,
    link_rows,
    link_target,
    link_weight,
    link_count,
):
    comps, vecs, sites = rand_vectors.shape
    fr = comps * vecs
    tiles, tile, _ = onsite.shape
    cap = link_rows.shape[1]
    slots = 2 * n * cap
    wide, tall = TC * tile, TR * tile
    vmem = pl.BlockSpec(memory_space=pltpu.VMEM)
    hbm = pl.BlockSpec(memory_space=pltpu.HBM)
    stage = pl.pallas_call(
        functools.partial(kernel, n, nl),
        out_shape=(
            pltpu.VMEM((fr, sites), BF16),
            pltpu.VMEM((fr, sites), F32),
            pltpu.VMEM((fr, sites), F32),
            pltpu.VMEM((slots, sites), BF16),
            pltpu.VMEM((2 * fr, slots), BF16),
            pltpu.VMEM((2, comps, sites), F32),
        ),
        in_specs=[hbm] * 10,
        out_specs=(vmem,) * 6,
        scratch_shapes=[
            pltpu.SMEM((2, tiles), jnp.int32),
            pltpu.VMEM((1, sites), F32),
            pltpu.VMEM((n, cap), jnp.int32),
            pltpu.VMEM((n, cap), jnp.int32),
            pltpu.VMEM((n, cap), BF16),
            pltpu.SMEM((n,), jnp.int32),
            pltpu.VMEM((tiles, tile, tile), BF16),
            pltpu.VMEM((tiles, tile, tile), BF16),
            pltpu.VMEM((tiles, tile, tile), BF16),
            pltpu.VMEM((fr, sites), BF16),
            pltpu.VMEM((slots, tile), jnp.int32),
            pltpu.VMEM((slots, 2 * fr), F32),
            pltpu.VMEM((slots, 2 * fr), F32),
            pltpu.VMEM((slots, 2 * fr), F32),
            pltpu.VMEM((n, cap), F32),
            pltpu.VMEM((2, n, 2 * cap, 2 * fr), BF16),
            pltpu.VMEM((2, n, 2 * cap, 2 * fr), BF16),
            pltpu.VMEM((2, fr, wide), BF16),
            pltpu.VMEM((2, fr, wide), BF16),
            pltpu.VMEM((2, fr, wide), BF16),
            pltpu.VMEM((2, fr, tall), BF16),
            pltpu.VMEM((2, fr, tall), BF16),
            pltpu.SemaphoreType.DMA((10,)),
            pltpu.SemaphoreType.DMA((2, n)),
            pltpu.SemaphoreType.DMA((2, n)),
            pltpu.SemaphoreType.DMA((2, 3)),
            pltpu.SemaphoreType.DMA((2, 3)),
        ],
        compiler_params=pltpu.CompilerParams(
            collective_id=0, has_side_effects=True, vmem_limit_bytes=30 * 1024 * 1024
        ),
    )(
        *[
            pltpu.with_memory_space_constraint(operand, pltpu.HBM)
            for operand in (
                rand_vectors.reshape(fr, sites),
                onsite,
                down_hop,
                right_hop,
                pattern.T,
                pairing.reshape(1, sites),
                link_rows,
                link_target,
                link_weight,
                link_count,
            )
        ]
    )
    one, two, moments = pl.pallas_call(
        finish,
        out_shape=(
            jax.ShapeDtypeStruct((fr, sites), F32),
            jax.ShapeDtypeStruct((fr, sites), F32),
            jax.ShapeDtypeStruct((3, comps, sites), F32),
        ),
        in_specs=[vmem] * 6,
        out_specs=(hbm,) * 3,
        scratch_shapes=[
            pltpu.VMEM((fr, sites), F32),
            pltpu.VMEM((comps, sites), F32),
            pltpu.SemaphoreType.DMA((3 + TR,)),
        ],
        compiler_params=pltpu.CompilerParams(vmem_limit_bytes=8 * 1024 * 1024),
    )(*stage)
    return (
        one.reshape(comps, vecs, sites),
        two.reshape(comps, vecs, sites),
        moments,
    )


def solution(mesh):
    spread = ("tile", "layer")
    in_specs = (
        P(None, None, spread),
        P(spread, None, None),
        P(spread, None, None),
        P(spread, None, None),
        P(spread, None),
        P(spread),
        P(spread, None),
        P(spread, None),
        P(spread, None),
        P(spread),
    )
    out_specs = (P(None, None, spread),) * 3
    return jax.shard_map(
        functools.partial(shards, mesh.shape["tile"], mesh.shape["layer"]),
        mesh=mesh,
        in_specs=in_specs,
        out_specs=out_specs,
        check_vma=False,
    )
```

```python
import functools

import jax
import jax.numpy as jnp
from jax import lax
from jax.experimental import pallas as pl
from jax.experimental.pallas import tpu as pltpu
from jax.sharding import PartitionSpec as P

TR = 4
TC = 6
MESH = pl.DeviceIdType.MESH
F32 = jnp.float32
BF16 = jnp.bfloat16


def dot_nn(a, b):
    return lax.dot_general(a, b, (((1,), (0,)), ((), ())), preferred_element_type=F32)


def dot_nt(a, b):
    return lax.dot_general(a, b, (((1,), (1,)), ((), ())), preferred_element_type=F32)


def mean(v, comps, vecs):
    return jnp.sum(v.reshape(comps, vecs, v.shape[1]), axis=1) * (1.0 / vecs)


def each(count, body):
    if count <= 16:
        for i in range(count):
            body(i)
    else:

        def step(i, carry):
            body(i)
            return carry

        lax.fori_loop(0, count, step, 0)


def kernel(
    n,
    nl,
    x_hbm,
    on_hbm,
    down_hbm,
    right_hbm,
    pat_hbm,
    pair_hbm,
    rows_hbm,
    target_hbm,
    weight_hbm,
    count_hbm,
    x_ref,
    one_ref,
    acc_ref,
    hot_ref,
    terms_ref,
    mom_ref,
    pat_ref,
    pair_ref,
    rows_ref,
    target_ref,
    weight_ref,
    count_ref,
    on_ref,
    down_ref,
    right_ref,
    oneb_ref,
    idx_ref,
    wsend_ref,
    wloc_ref,
    gath_ref,
    meet_ref,
    parts_ref,
    wide_ref,
    sbuf,
    lbuf,
    pbuf,
    low_in,
    up_in,
    cbuf,
    col_in,
    load_sem,
    link_send,
    link_recv,
    edge_send,
    edge_recv,
):
    t = lax.axis_index("tile")
    l = lax.axis_index("layer")
    far = lax.rem(l + nl // 2, nl)
    is_left = lax.rem(l, 2) == 0
    partner = l + 1 - 2 * lax.rem(l, 2)
    fr, sites = x_ref.shape
    tile = on_ref.shape[1]
    tiles = sites // tile
    cap = rows_ref.shape[1]
    slots = n * 2 * cap
    wide = TC * tile

    has_up = t > 0
    has_low = t < n - 1
    barrier = pltpu.get_barrier_semaphore()
    each(
        n,
        lambda s: pl.semaphore_signal(barrier, inc=1, device_id=(s, far), device_id_type=MESH),
    )
    pl.semaphore_signal(barrier, inc=1, device_id=(t, partner), device_id_type=MESH)

    @pl.when(has_up)
    def _():
        pl.semaphore_signal(barrier, inc=1, device_id=(t - 1, l), device_id_type=MESH)

    @pl.when(has_low)
    def _():
        pl.semaphore_signal(barrier, inc=1, device_id=(t + 1, l), device_id_type=MESH)

    moved = (
        (rows_hbm, rows_ref),
        (target_hbm, target_ref),
        (weight_hbm, weight_ref),
        (count_hbm, count_ref),
        (x_hbm, x_ref),
        (pat_hbm, pat_ref),
        (down_hbm, down_ref),
        (right_hbm, right_ref),
        (on_hbm, on_ref),
        (pair_hbm, pair_ref),
    )
    loads = [pltpu.make_async_copy(a, b, load_sem.at[i]) for i, (a, b) in enumerate(moved)]
    for load in loads:
        load.start()

    @pl.when(jnp.logical_not(has_up))
    def _():
        up_in[...] = jnp.zeros_like(up_in)

    @pl.when(jnp.logical_not(has_low))
    def _():
        low_in[...] = jnp.zeros_like(low_in)

    for load in loads[0:4]:
        load.wait()

    sub = lax.broadcasted_iota(jnp.int32, (cap, cap), 0)
    lane = lax.broadcasted_iota(jnp.int32, (cap, cap), 1)
    eye = sub == lane
    half = lax.broadcasted_iota(jnp.int32, (cap, 2 * fr), 1) >= fr

    wide_ref[...] = weight_ref[...].astype(F32)

    def columns(s):
        def column(row):
            spread = jnp.broadcast_to(row.astype(F32), (cap, cap))
            return jnp.sum(jnp.where(eye, spread, 0.0), axis=1, keepdims=True)

        base = s * (2 * cap)
        out_col = column(rows_ref[pl.ds(s, 1), :])
        own_col = column(target_ref[pl.ds(s, 1), :])
        idx_ref[pl.ds(base, cap), :] = jnp.broadcast_to(out_col, (cap, tile)).astype(jnp.int32)
        idx_ref[pl.ds(base + cap, cap), :] = jnp.broadcast_to(own_col, (cap, tile)).astype(
            jnp.int32
        )
        live = lax.broadcasted_iota(jnp.int32, (1, cap), 1) < count_ref[s]
        w_col = column(jnp.where(live, wide_ref[pl.ds(s, 1), :], 0.0))
        w_wide = jnp.where(half, jnp.broadcast_to(w_col, (cap, 2 * fr)), 0.0)
        zero = jnp.zeros_like(w_wide)
        wsend_ref[pl.ds(base, cap), :] = w_wide
        wsend_ref[pl.ds(base + cap, cap), :] = zero
        wloc_ref[pl.ds(base, cap), :] = zero
        wloc_ref[pl.ds(base + cap, cap), :] = w_wide

    each(n, columns)
    gath_ref[...] = jnp.zeros_like(gath_ref)

    lanes = lax.broadcasted_iota(jnp.int32, (slots, tile), 1)
    for p in range(tiles):
        hot = jnp.where(idx_ref[...] == lanes + p * tile, 1.0, 0.0)
        hot_ref[:, p * tile : (p + 1) * tile] = hot.astype(BF16)

    def block(ref, p):
        return ref[:, p * tile : (p + 1) * tile]

    def link_copy(rd, s, mine):
        return pltpu.make_async_remote_copy(
            src_ref=sbuf.at[rd, s],
            dst_ref=lbuf.at[rd, mine],
            send_sem=link_send.at[rd, s],
            recv_sem=link_recv.at[rd, mine],
            device_id=(s, far),
            device_id_type=MESH,
        )

    def field_copy(rd, src):
        return pltpu.make_async_remote_copy(
            src_ref=src.at[:, 0:wide],
            dst_ref=low_in.at[rd],
            send_sem=edge_send.at[rd, 0],
            recv_sem=edge_recv.at[rd, 0],
            device_id=(t - 1, l),
            device_id_type=MESH,
        )

    def partial_copy(rd):
        return pltpu.make_async_remote_copy(
            src_ref=pbuf.at[rd],
            dst_ref=up_in.at[rd],
            send_sem=edge_send.at[rd, 1],
            recv_sem=edge_recv.at[rd, 1],
            device_id=(t + 1, l),
            device_id_type=MESH,
        )

    def column_copy(rd):
        return pltpu.make_async_remote_copy(
            src_ref=cbuf.at[rd],
            dst_ref=col_in.at[rd],
            send_sem=edge_send.at[rd, 2],
            recv_sem=edge_recv.at[rd, 2],
            device_id=(t, partner),
            device_id_type=MESH,
        )

    def gather(src):
        gath_ref[:, 0:fr] = dot_nt(hot_ref[...], src[...])

    def fill_links(rd):
        def fill(s):
            base = s * (2 * cap)
            both = jnp.concatenate(
                [gath_ref[pl.ds(base + cap, cap), :], gath_ref[pl.ds(base, cap), :]], axis=0
            )
            sbuf[rd, s] = (both + wsend_ref[pl.ds(base, 2 * cap), :]).astype(BF16)

        each(n, fill)

    def meets():
        step = tile if slots % tile == 0 else slots
        count = slots // step

        def meet(i, j):
            rows = pl.ds(pl.multiple_of(i * step, step), step)
            cols = pl.ds(pl.multiple_of(j * step, step), step)
            meet_ref[rows, cols] = dot_nt(hot_ref[rows, :], hot_ref[cols, :]).astype(BF16)

        if count == 1:
            meet_ref[...] = dot_nt(hot_ref[...], hot_ref[...]).astype(BF16)
        else:
            each(count, lambda i: lax.fori_loop(0, count, lambda j, c: (meet(i, j), c)[1], 0))

    def edges(rd, src):
        for k in range(TC):
            p = (TR - 1) * TC + k
            pbuf[rd, :, k * tile : (k + 1) * tile] = dot_nn(block(src, p), down_ref[p]).astype(
                BF16
            )
        for r in range(TR):
            p = r * TC + TC - 1
            passed = dot_nn(block(src, p), right_ref[p])
            own = block(src, r * TC).astype(F32)
            cbuf[rd, :, r * tile : (r + 1) * tile] = jnp.where(is_left, passed, own).astype(BF16)

    def send_links(rd):
        each(n, lambda s: link_copy(rd, s, t).start())

    def send_edges(rd, src):
        column_copy(rd).start()

        @pl.when(has_up)
        def _():
            field_copy(rd, src).start()

        @pl.when(has_low)
        def _():
            partial_copy(rd).start()

    def local(src):
        for r in range(TR):
            for k in range(TC):
                p = r * TC + k
                ins = [block(src, p)]
                mats = [on_ref[p]]
                if r > 0:
                    ins.append(block(src, p - TC))
                    mats.append(down_ref[p - TC])
                if k > 0:
                    ins.append(block(src, p - 1))
                    mats.append(right_ref[p - 1])
                total = dot_nn(jnp.concatenate(ins, axis=1), jnp.concatenate(mats, axis=0))
                ins, mats = [], []
                if r < TR - 1:
                    ins.append(block(src, p + TC))
                    mats.append(down_ref[p])
                if k < TC - 1:
                    ins.append(block(src, p + 1))
                    mats.append(right_ref[p])
                if ins:
                    total = total + dot_nt(
                        jnp.concatenate(ins, axis=1), jnp.concatenate(mats, axis=1)
                    )
                acc_ref[:, p * tile : (p + 1) * tile] = total

    def receive_edges(rd):
        @pl.when(has_low)
        def _():
            field_copy(rd, x_ref).wait_recv()

        @pl.when(has_up)
        def _():
            partial_copy(rd).wait_recv()

        column_copy(rd).wait_recv()

    def add_edges(rd):
        for k in range(TC):
            cols = slice(k * tile, (k + 1) * tile)
            acc_ref[:, cols] += up_in[rd, :, cols].astype(F32)
            p = (TR - 1) * TC + k
            acc_ref[:, p * tile : (p + 1) * tile] += dot_nt(low_in[rd, :, cols], down_ref[p])
        for r in range(TR):
            arrived = col_in[rd, :, r * tile : (r + 1) * tile].astype(F32)
            p = r * TC
            acc_ref[:, p * tile : (p + 1) * tile] += jnp.where(is_left, 0.0, arrived)
            p = r * TC + TC - 1
            field = jnp.where(is_left, arrived, 0.0).astype(BF16)
            acc_ref[:, p * tile : (p + 1) * tile] += dot_nt(field, right_ref[p])

    def link_terms(rd):
        each(n, lambda s: link_copy(rd, s, s).wait_recv())
        landed = lbuf[rd].reshape(slots, 2 * fr).astype(F32) + wloc_ref[...]
        turned = landed.T
        terms = turned[0:fr] * turned[fr : 2 * fr]
        high = terms.astype(BF16)
        low = (terms - high.astype(F32)).astype(BF16)
        return jnp.concatenate([high, low], axis=0)

    sign = jnp.where(lax.broadcasted_iota(jnp.int32, (fr, tile), 0) < fr // 2, 1.0, -1.0)

    def flipped(v):
        return jnp.concatenate([v[fr // 2 :], v[: fr // 2]], axis=0)

    def scattered(terms, p):
        both = dot_nn(terms, block(hot_ref, p))
        return both[0:fr] + both[fr : 2 * fr]

    loads[4].wait()
    gather(x_ref)
    fill_links(0)
    for load in loads[5:8]:
        load.wait()
    for p in range(tiles):
        down_ref[p] = down_ref[p] * pat_ref[0, p].astype(F32).astype(BF16)
        right_ref[p] = right_ref[p] * pat_ref[1, p].astype(F32).astype(BF16)
    edges(0, x_ref)
    pl.semaphore_wait(barrier, n + 1 + has_up.astype(jnp.int32) + has_low.astype(jnp.int32))
    send_links(0)
    send_edges(0, x_ref)
    loads[8].wait()
    loads[9].wait()
    local(x_ref)
    meets()
    receive_edges(0)
    add_edges(0)
    for p in range(tiles):
        cols = slice(p * tile, (p + 1) * tile)
        start = x_ref[:, cols].astype(F32)
        value = sign * acc_ref[:, cols] + pair_ref[:, cols] * flipped(start)
        acc_ref[:, cols] = value
        for i in range(3):
            part = value.astype(BF16)
            parts_ref[i * fr : (i + 1) * fr, cols] = part
            value = value - part.astype(F32)
    three = dot_nt(parts_ref[...], hot_ref[...])
    at_slots = three[0:fr] + three[fr : 2 * fr] + three[2 * fr :]
    terms = link_terms(0)
    both = dot_nn(terms, meet_ref[...])
    met = both[0:fr] + both[fr : 2 * fr]
    signs = jnp.where(lax.broadcasted_iota(jnp.int32, (fr, slots), 0) < fr // 2, 1.0, -1.0)
    ends = at_slots + signs * met
    gath_ref[...] = jnp.concatenate([ends, jnp.zeros_like(ends)], axis=0).T
    fill_links(1)
    send_links(1)
    for p in range(tiles):
        cols = slice(p * tile, (p + 1) * tile)
        one = acc_ref[:, cols] + sign * scattered(terms, p)
        one_ref[:, cols] = one
        oneb_ref[:, cols] = one.astype(BF16)

    edges(1, oneb_ref)
    send_edges(1, oneb_ref)
    local(oneb_ref)
    comps, vecs = mom_ref.shape[1], fr // mom_ref.shape[1]
    for p in range(tiles):
        cols = slice(p * tile, (p + 1) * tile)
        start = x_ref[:, cols].astype(F32)
        mom_ref[0, :, cols] = mean(start * start, comps, vecs)
        mom_ref[1, :, cols] = mean(start * one_ref[:, cols], comps, vecs)
    receive_edges(1)
    add_edges(1)
    for p in range(tiles):
        cols = slice(p * tile, (p + 1) * tile)
        start = x_ref[:, cols].astype(F32)
        own = sign * acc_ref[:, cols] + pair_ref[:, cols] * flipped(one_ref[:, cols])
        acc_ref[:, cols] = 2.0 * own - start
    terms_ref[...] = link_terms(1)

    for rd in range(2):
        each(n, lambda s: link_copy(rd, s, t).wait_send())
        column_copy(rd).wait_send()

        @pl.when(has_up)
        def _():
            field_copy(rd, x_ref).wait_send()

        @pl.when(has_low)
        def _():
            partial_copy(rd).wait_send()


def finish(
    x_ref,
    one_ref,
    acc_ref,
    hot_ref,
    terms_ref,
    mom_ref,
    one_out,
    two_out,
    mom_out,
    two_ref,
    last_ref,
    sem,
):
    fr, sites = x_ref.shape
    comps, vecs = mom_ref.shape[1], fr // mom_ref.shape[1]
    tile = sites // (TR * TC)
    wide = TC * tile
    copies = [
        pltpu.make_async_copy(one_ref, one_out, sem.at[0]),
        pltpu.make_async_copy(mom_ref, mom_out.at[0:2], sem.at[1]),
    ]
    for copy in copies:
        copy.start()
    sign = jnp.where(lax.broadcasted_iota(jnp.int32, (fr, tile), 0) < fr // 2, 2.0, -2.0)
    terms = terms_ref[...]
    for r in range(TR):
        for k in range(TC):
            p = r * TC + k
            cols = slice(p * tile, (p + 1) * tile)
            both = dot_nn(terms, hot_ref[:, cols])
            two = acc_ref[:, cols] + sign * (both[0:fr] + both[fr : 2 * fr])
            two_ref[:, cols] = two
            last_ref[:, cols] = mean(x_ref[:, cols].astype(F32) * two, comps, vecs)
        row = slice(r * wide, (r + 1) * wide)
        copy = pltpu.make_async_copy(two_ref.at[:, row], two_out.at[:, row], sem.at[2 + r])
        copy.start()
        copies.append(copy)
    copy = pltpu.make_async_copy(last_ref, mom_out.at[2], sem.at[2 + TR])
    copy.start()
    copies.append(copy)
    for copy in copies:
        copy.wait()


def shards(
    n,
    nl,
    rand_vectors,
    onsite,
    down_hop,
    right_hop,
    pattern,
    pairing,
    link_rows,
    link_target,
    link_weight,
    link_count,
):
    comps, vecs, sites = rand_vectors.shape
    fr = comps * vecs
    tiles, tile, _ = onsite.shape
    cap = link_rows.shape[1]
    slots = 2 * n * cap
    wide, tall = TC * tile, TR * tile
    vmem = pl.BlockSpec(memory_space=pltpu.VMEM)
    hbm = pl.BlockSpec(memory_space=pltpu.HBM)
    stage = pl.pallas_call(
        functools.partial(kernel, n, nl),
        out_shape=(
            pltpu.VMEM((fr, sites), BF16),
            pltpu.VMEM((fr, sites), F32),
            pltpu.VMEM((fr, sites), F32),
            pltpu.VMEM((slots, sites), BF16),
            pltpu.VMEM((2 * fr, slots), BF16),
            pltpu.VMEM((2, comps, sites), F32),
        ),
        in_specs=[hbm] * 10,
        out_specs=(vmem,) * 6,
        scratch_shapes=[
            pltpu.SMEM((2, tiles), jnp.int32),
            pltpu.VMEM((1, sites), F32),
            pltpu.VMEM((n, cap), jnp.int32),
            pltpu.VMEM((n, cap), jnp.int32),
            pltpu.VMEM((n, cap), BF16),
            pltpu.SMEM((n,), jnp.int32),
            pltpu.VMEM((tiles, tile, tile), BF16),
            pltpu.VMEM((tiles, tile, tile), BF16),
            pltpu.VMEM((tiles, tile, tile), BF16),
            pltpu.VMEM((fr, sites), BF16),
            pltpu.VMEM((slots, tile), jnp.int32),
            pltpu.VMEM((slots, 2 * fr), F32),
            pltpu.VMEM((slots, 2 * fr), F32),
            pltpu.VMEM((slots, 2 * fr), F32),
            pltpu.VMEM((slots, slots), BF16),
            pltpu.VMEM((3 * fr, sites), BF16),
            pltpu.VMEM((n, cap), F32),
            pltpu.VMEM((2, n, 2 * cap, 2 * fr), BF16),
            pltpu.VMEM((2, n, 2 * cap, 2 * fr), BF16),
            pltpu.VMEM((2, fr, wide), BF16),
            pltpu.VMEM((2, fr, wide), BF16),
            pltpu.VMEM((2, fr, wide), BF16),
            pltpu.VMEM((2, fr, tall), BF16),
            pltpu.VMEM((2, fr, tall), BF16),
            pltpu.SemaphoreType.DMA((10,)),
            pltpu.SemaphoreType.DMA((2, n)),
            pltpu.SemaphoreType.DMA((2, n)),
            pltpu.SemaphoreType.DMA((2, 3)),
            pltpu.SemaphoreType.DMA((2, 3)),
        ],
        compiler_params=pltpu.CompilerParams(
            collective_id=0, has_side_effects=True, vmem_limit_bytes=44 * 1024 * 1024
        ),
    )(
        *[
            pltpu.with_memory_space_constraint(operand, pltpu.HBM)
            for operand in (
                rand_vectors.reshape(fr, sites),
                onsite,
                down_hop,
                right_hop,
                pattern.T,
                pairing.reshape(1, sites),
                link_rows,
                link_target,
                link_weight,
                link_count,
            )
        ]
    )
    one, two, moments = pl.pallas_call(
        finish,
        out_shape=(
            jax.ShapeDtypeStruct((fr, sites), F32),
            jax.ShapeDtypeStruct((fr, sites), F32),
            jax.ShapeDtypeStruct((3, comps, sites), F32),
        ),
        in_specs=[vmem] * 6,
        out_specs=(hbm,) * 3,
        scratch_shapes=[
            pltpu.VMEM((fr, sites), F32),
            pltpu.VMEM((comps, sites), F32),
            pltpu.SemaphoreType.DMA((3 + TR,)),
        ],
        compiler_params=pltpu.CompilerParams(vmem_limit_bytes=8 * 1024 * 1024),
    )(*stage)
    return (
        one.reshape(comps, vecs, sites),
        two.reshape(comps, vecs, sites),
        moments,
    )


def solution(mesh):
    spread = ("tile", "layer")
    in_specs = (
        P(None, None, spread),
        P(spread, None, None),
        P(spread, None, None),
        P(spread, None, None),
        P(spread, None),
        P(spread),
        P(spread, None),
        P(spread, None),
        P(spread, None),
        P(spread),
    )
    out_specs = (P(None, None, spread),) * 3
    return jax.shard_map(
        functools.partial(shards, mesh.shape["tile"], mesh.shape["layer"]),
        mesh=mesh,
        in_specs=in_specs,
        out_specs=out_specs,
        check_vma=False,
    )
```
